32 devices in a mesh: blk: 4 (over z), tok: 8 (over y, x, core).
Axes of the slice: x: 2, y: 2, z: 4, core: 2. Of those that a mesh axis runs over, the one named last changes fastest.
Arguments:
- inputs: float32 [2048, 16384], P('tok', 'blk'), may hold values from -6 to 6
- first_factor: float32 [16, 1024, 1024], P('blk', 'tok'), may hold values from -0.1875 to 0.1875
- second_factor: float32 [16, 1024, 1024], P('blk', 'tok'), may hold values from -0.1875 to 0.1875
- cotangent: float32 [2048, 16384], P('tok', 'blk'), may hold values from -6 to 6
Outputs:
- input_grad: float32 [2048, 16384], P('tok', 'blk')
- first_grad: float32 [16, 1024, 1024], P('blk', 'tok')
- second_grad: float32 [16, 1024, 1024], P('blk', 'tok')
The draws below stay inside these ranges and needn't reach their ends.
All inputs are finite; a program needn't handle non-finite values.
Results may differ from the reference program's by a relative error of at most 0.00013.
Values sent between devices are 32-bit elements; how exact they have to be, the bound alone decides.
No kernel may reach another device: no remote copies, remote signals or barrier semaphores. Data moves between devices by JAX's collectives and lax.ppermute only.
A program may use at most 128 MiB of HBM per device.

```python
import jax
import jax.numpy as jnp
from jax import lax

BLOCKS = 16
BS = 1024
FEATURES = 16384
TOKENS = 2048


def level_of(rng, dims, pieces, least, largest):
    def one(dim, parts):
        draws = jax.random.uniform(jax.random.fold_in(jax.random.fold_in(rng, 6), dim), (parts,), jnp.float32, least / len(pieces), largest / len(pieces))
        return jnp.repeat(jnp.exp(draws), dims[dim] // parts).reshape((-1,) + (1,) * (len(dims) - dim - 1))

    level = one(*pieces[0])
    for cut in pieces[1:]:
        level = level * one(*cut)
    return level


def centred(stream_key, shape, width, most, pieces=(), dtype=jnp.bfloat16):
    entries = jax.random.normal(stream_key, shape, jnp.float32) * width
    if len(pieces) > 0:
        entries = level_of(stream_key, shape, pieces, -0.22, 0.18) * entries
    return jnp.clip(entries, min=-most, max=most).astype(dtype)


def setup_inputs(seed: int = 0) -> dict:
    key_of = jax.random.split(jax.random.key(seed), 5)
    return {
        "inputs": centred(key_of[0], (TOKENS, FEATURES), 1.0, 6.0, ((0, 8), (1, 4)), jnp.float32),
        "first_factor": centred(key_of[1], (BLOCKS, BS, BS), BS ** -0.5, 0.1875, ((0, 4), (1, 8)), jnp.float32),
        "second_factor": centred(key_of[2], (BLOCKS, BS, BS), BS ** -0.5, 0.1875, ((0, 4), (1, 8)), jnp.float32),
        "cotangent": centred(key_of[3], (TOKENS, FEATURES), 1.0, 6.0, ((0, 8), (1, 4)), jnp.float32),
    }


def forward(inputs, first_factor, second_factor):
    hp = lax.Precision.HIGHEST
    count = inputs.shape[0]
    group = BS // BLOCKS
    xb = inputs.reshape(count, BLOCKS, BS)
    first = jnp.einsum('tbi,bio->tbo', xb, first_factor, precision=hp)
    mixed = first.reshape(count, BLOCKS, BLOCKS, group).transpose(0, 2, 1, 3).reshape(count, BLOCKS, BS)
    second = jnp.einsum('tsk,sko->tso', mixed, second_factor, precision=hp)
    return jax.nn.gelu(second, approximate=False).reshape(count, BLOCKS * BS)

def reference(inputs, first_factor, second_factor, cotangent):
    outputs, pullback = jax.vjp(forward, inputs, first_factor, second_factor)
    input_grad, first_grad, second_grad = pullback(cotangent)
    return (input_grad, first_grad, second_grad)
```

```python
import functools
import math

import jax
import jax.numpy as jnp
from jax import lax
from jax.experimental import pallas as pl
from jax.experimental.pallas import tpu as pltpu
from jax.sharding import PartitionSpec as P


F32 = jnp.float32
BF16 = jnp.bfloat16
LANES = 128


def split(value):
    high = value.astype(BF16)
    return high, (value - high.astype(F32)).astype(BF16)


def product(left, right, dims):
    def one(a, b):
        return lax.dot_general(a, b, (dims, ((), ())), preferred_element_type=F32)

    return one(left[0], right[1]) + one(left[1], right[0]) + one(left[0], right[0])


PLAIN = ((1,), (0,))
TURNED = ((1,), (1,))


def swap_groups(first, second):
    half = LANES // 2
    low = lax.broadcasted_iota(jnp.int32, first.shape, 1) < half
    return (
        jnp.where(low, first, pltpu.roll(second, half, 1)),
        jnp.where(low, pltpu.roll(first, half, 1), second),
    )


def place_rows(pieces, me, high, low):
    for p, piece in enumerate(pieces):
        rows = piece.shape[0]
        at = pl.ds(pl.multiple_of((me ^ p) * rows, rows), rows)
        h, l = split(piece[...])
        high[at, :] = h
        low[at, :] = l


def place_turned(value, first_shard, me, rows, high, low):
    turned = value.T
    h, l = split(turned)
    for u in range(turned.shape[0] // rows):
        at = pl.ds(pl.multiple_of(((first_shard + u) ^ me) * rows, rows), rows)
        high[at, :] = h[u * rows : (u + 1) * rows]
        low[at, :] = l[u * rows : (u + 1) * rows]


def forward_kernel(T, Z, ids, x_ref, *refs):
    pieces = (refs[:T], refs[T : 2 * T])
    outs = refs[2 * T : 2 * T + Z]
    xh, xl, fh, fl = refs[2 * T + Z :]
    me = ids[0]
    step = pl.program_id(0)
    order = x_ref.shape[1] // 2

    @pl.when(step == 0)
    def _():
        h, l = split(x_ref[...])
        xh[...] = h
        xl[...] = l

    results = []
    for i in range(2):
        place_rows(pieces[i], me, fh.at[i], fl.at[i])
        at = slice(i * order, (i + 1) * order)
        results.append(product((xh[:, at], xl[:, at]), (fh[i], fl[i]), PLAIN))
    for c in range(Z):

        @pl.when(step == c)
        def _():
            for h in range(results[0].shape[1] // LANES):
                at = slice(h * LANES, (h + 1) * LANES)
                one, two = swap_groups(results[0][:, at], results[1][:, at])
                outs[c][2 * h] = one
                outs[c][2 * h + 1] = two


def middle_kernel(T, Z, chunks, ids, *refs):
    arrived = refs[: Z * chunks]
    refs = refs[Z * chunks :]
    pieces = (refs[:T], refs[T : 2 * T])
    cots = refs[2 * T : 2 * T + 2]
    odd, even = refs[2 * T + 2 : 2 * T + 4]
    outs = refs[2 * T + 4 : 2 * T + 4 + Z]
    mh, ml, th, tl, sh, sl, back = refs[2 * T + 4 + Z :]
    me, z = ids[0], ids[1]
    rows = pieces[0][0].shape[0]
    step = pl.program_id(0)

    @pl.when(step == 0)
    def _():
        for c in range(Z):
            source = lax.rem(z + (Z - c), Z)
            for k in range(chunks):
                q = source * chunks + k
                for i in range(2):
                    value = arrived[c * chunks + k][i]
                    h, l = split(value)
                    at = pl.ds(pl.multiple_of(q * LANES, LANES), LANES)
                    mh[i, :, at] = h
                    ml[i, :, at] = l
                    place_turned(value, q * (LANES // rows), me, rows, th.at[i], tl.at[i])
        back[...] = jnp.zeros_like(back)

    for i in range(2):
        place_rows(pieces[i], me, sh.at[i], sl.at[i])
        factor = (sh[i], sl[i])
        second = product((mh[i], ml[i]), factor, PLAIN)
        cdf = 0.5 * (1.0 + lax.erf(second * (1.0 / math.sqrt(2.0))))
        density = jnp.exp(-0.5 * second * second) * (1.0 / math.sqrt(2.0 * math.pi))
        delta = split(cots[i][...] * (cdf + second * density))
        grad = product((th[i], tl[i]), delta, PLAIN)
        for p in range(T):
            (odd if p % 2 else even)[i, p // 2] = grad[p * rows : (p + 1) * rows]
        back[i] += product(delta, factor, TURNED)

    @pl.when(step == pl.num_programs(0) - 1)
    def _():
        width = outs[0].shape[0] * LANES // 2
        for c in range(Z):
            start = lax.rem(z + c, Z) * width
            for h in range(width // LANES):
                at = pl.ds(pl.multiple_of(start + h * LANES, LANES), LANES)
                one, two = swap_groups(back[0, :, at], back[1, :, at])
                outs[c][2 * h] = one
                outs[c][2 * h + 1] = two


def backward_kernel(T, Z, chunks, tile, ids, _, x_ref, *refs):
    arrived = refs[: Z * chunks]
    refs = refs[Z * chunks :]
    pieces = (refs[:T], refs[T : 2 * T])
    out, odd, even = refs[2 * T : 2 * T + 3]
    dh, dl, th, tl, fh, fl = refs[2 * T + 3 :]
    me, z = ids[0], ids[1]
    rows = pieces[0][0].shape[0]
    order = x_ref.shape[1] // 2
    step = pl.program_id(0)

    @pl.when(step == 0)
    def _():
        for c in range(Z):
            source = lax.rem(z + (Z - c), Z)
            for k in range(chunks):
                q = source * chunks + k
                at = pl.ds(pl.multiple_of(q * LANES, LANES), LANES)
                for i in range(2):
                    h, l = split(arrived[c * chunks + k][i])
                    dh[i, :, at] = h
                    dl[i, :, at] = l
        for i in range(2):
            for q in range(order // LANES):
                start = i * order + q * LANES
                value = x_ref[:, start : start + LANES]
                place_turned(value, q * (LANES // rows), me, rows, th.at[i], tl.at[i])
        out[...] = jnp.zeros_like(out)

    for i in range(2):
        place_rows(pieces[i], me, fh.at[i], fl.at[i])
        at = pl.ds(pl.multiple_of(step * tile, tile), tile)
        delta = (dh[i, :, at], dl[i, :, at])
        grad = product((th[i], tl[i]), delta, PLAIN)
        for p in range(T):
            (odd if p % 2 else even)[i, p // 2] = grad[p * rows : (p + 1) * rows]
        out[:, i * order : (i + 1) * order] += product(delta, (fh[i], fl[i]), TURNED)


def cost(flops, moved):
    return pl.CostEstimate(flops=flops, bytes_accessed=moved, transcendentals=0)


def params():
    return pltpu.CompilerParams(
        dimension_semantics=("arbitrary",), vmem_limit_bytes=48 * 1024 * 1024
    )


def kernel(*args, **settings):
    return pl.pallas_call(*args, **settings)


def body(inputs, first_factor, second_factor, cotangent):
    T, Z = lax.axis_size("tok"), lax.axis_size("blk")
    LB, rows, order = first_factor.shape
    count = inputs.shape[0]
    group = order // (LB * Z)
    chunks = LB // 2
    width = LB * group
    tile = 256
    steps = order // tile
    half = T // 2
    ids = jnp.stack([lax.axis_index("tok"), lax.axis_index("blk")]).astype(jnp.int32)
    bits = [1 << k for k in range(1, T.bit_length() - 1)]

    def across(value, bit):
        return lax.ppermute(value, "tok", [(d, d ^ bit) for d in range(T)])

    def along(value, c):
        return lax.ppermute(value, "blk", [(d, (d + c) % Z) for d in range(Z)])

    def gather(factor, after=None):
        blocks, last = [], []
        for b in range(LB):
            shard = factor[b]
            if after is not None:
                shard, _ = lax.optimization_barrier((shard, after[0]))
            held = {0: shard}
            for bit in bits if b % 2 == 0 else bits[::-1]:
                held.update({p | bit: across(v, bit) for p, v in list(held.items())})
            last.append(held[T - 2])
            held.update({p | 1: across(v, 1) for p, v in list(held.items())})
            blocks.append([held[p] for p in range(T)])
        return blocks, [(last[2 * k], last[2 * k + 1]) for k in range(chunks)]

    def scatter(odd, even):
        met = across(odd, 1)
        terms = [
            {p: [(even, (i, p // 2)), (met, (i, p // 2))] for p in range(0, T, 2)}
            for i in range(2)
        ]
        sums = None
        for n in range(len(bits)):
            going, sums = [], []
            for i, bit in enumerate((bits[n], bits[::-1][n])):
                going.append([p for p in terms[i] if p & bit])
                sums.append(jnp.stack([total(terms[i].pop(p)) for p in going[i]]))
            sums = lax.optimization_barrier(sums)
            for i, bit in enumerate((bits[n], bits[::-1][n])):
                sent = across(sums[i], bit)
                for m, p in enumerate(going[i]):
                    terms[i][p ^ bit].append((sent, m))
        return [terms[i][0] for i in range(2)], sums

    def total(found):
        return functools.reduce(jnp.add, [array[at] for array, at in found])

    def settle(parts, after):
        arrays = [[[array for array, _ in found] for found in part] for part in parts]
        arrays, _ = lax.optimization_barrier((arrays, after))
        sums = []
        for part, held in zip(parts, arrays):
            for found, group in zip(part, held):
                sums.append(total([(array, at) for array, (_, at) in zip(group, found)]))
        return jnp.stack(sums)

    def full(shape):
        return pl.BlockSpec(shape, lambda n, ids: (0,) * len(shape))

    first_pieces, last = gather(first_factor)
    second_pieces, _ = gather(second_factor, last)

    flops = 2 * 2 * count * order * order
    column = pl.BlockSpec((rows, tile), lambda n, ids: (0, n))

    def exchange(sent):
        arrived = []
        for c in range(Z):
            if c == 0:
                arrived.append([(sent[c], j) for j in range(chunks)])
            elif 2 * c == Z and Z % 4 == 0 and chunks == 2:
                near = along(sent[c][:2], c)
                far = along(sent[c][2:], Z - c // 2)
                far = along(far, Z - c // 2)
                arrived.append([(near, 0), (far, 0)])
            else:
                whole = along(sent[c], c)
                arrived.append([(whole, j) for j in range(chunks)])
        return arrived

    def arrivals(exchanged, j):
        found = [exchanged[k][c][j] for c in range(Z) for k in range(chunks)]
        specs = [
            pl.BlockSpec((2, count, LANES), lambda n, ids, at=at: (at, 0, 0)) for _, at in found
        ]
        return [array for array, _ in found], specs

    mixed = []
    for k in range(chunks):
        sent = kernel(
            functools.partial(forward_kernel, T, Z),
            grid_spec=pltpu.PrefetchScalarGridSpec(
                num_scalar_prefetch=1,
                grid=(Z,),
                in_specs=[pl.BlockSpec((count, 2 * order), lambda n, ids, k=k: (0, k))]
                + [pl.BlockSpec((rows, width), lambda n, ids: (0, lax.rem(ids[1] + n, Z)))]
                * (2 * T),
                out_specs=[full((LB, count, LANES))] * Z,
                scratch_shapes=[pltpu.VMEM((count, 2 * order), BF16)] * 2
                + [pltpu.VMEM((2, order, width), BF16)] * 2,
            ),
            out_shape=[jax.ShapeDtypeStruct((LB, count, LANES), F32)] * Z,
            compiler_params=params(),
            cost_estimate=cost(3 * flops, 4 * 2 * (order * order + 2 * count * order)),
        )(ids, inputs, *first_pieces[2 * k], *first_pieces[2 * k + 1])
        mixed.append(exchange(sent))

    returned = []
    second_parts = []
    for k in range(chunks):
        arrays, specs = arrivals(mixed, k)
        odd, even, *sent = kernel(
            functools.partial(middle_kernel, T, Z, chunks),
            grid_spec=pltpu.PrefetchScalarGridSpec(
                num_scalar_prefetch=1,
                grid=(steps,),
                in_specs=specs
                + [column] * (2 * T)
                + [
                    pl.BlockSpec((count, tile), lambda n, ids, b=b: (0, b * steps + n))
                    for b in (2 * k, 2 * k + 1)
                ],
                out_specs=[pl.BlockSpec((2, half, rows, tile), lambda n, ids: (0, 0, 0, n))] * 2
                + [full((LB, count, LANES))] * Z,
                scratch_shapes=[pltpu.VMEM((2, count, order), BF16)] * 2
                + [pltpu.VMEM((2, order, count), BF16)] * 2
                + [pltpu.VMEM((2, order, tile), BF16)] * 2
                + [pltpu.VMEM((2, count, order), F32)],
            ),
            out_shape=[jax.ShapeDtypeStruct((2, half, rows, order), F32)] * 2
            + [jax.ShapeDtypeStruct((LB, count, LANES), F32)] * Z,
            compiler_params=params(),
            cost_estimate=cost(9 * flops, 4 * 2 * (2 * order * order + 3 * count * order)),
        )(
            ids,
            *arrays,
            *second_pieces[2 * k],
            *second_pieces[2 * k + 1],
            cotangent,
            cotangent,
        )
        returned.append(exchange(sent))
        second_parts.append(scatter(odd, even)[0])

    first_parts = []
    input_grad = None
    for k in range(chunks):
        arrays, specs = arrivals(returned, k)
        args = (inputs, *arrays, *first_pieces[2 * k], *first_pieces[2 * k + 1])
        before = ids if input_grad is None else input_grad
        input_grad, odd, even = kernel(
            functools.partial(backward_kernel, T, Z, chunks, tile),
            grid_spec=pltpu.PrefetchScalarGridSpec(
                num_scalar_prefetch=1,
                grid=(steps,),
                in_specs=[pl.BlockSpec(memory_space=pl.ANY)]
                + [pl.BlockSpec((count, 2 * order), lambda n, ids, k=k: (0, k))]
                + specs
                + [column] * (2 * T),
                out_specs=[pl.BlockSpec((count, 2 * order), lambda n, ids, k=k: (0, k))]
                + [pl.BlockSpec((2, half, rows, tile), lambda n, ids: (0, 0, 0, n))] * 2,
                scratch_shapes=[pltpu.VMEM((2, count, order), BF16)] * 2
                + [pltpu.VMEM((2, order, count), BF16)] * 2
                + [pltpu.VMEM((2, order, tile), BF16)] * 2,
            ),
            out_shape=[jax.ShapeDtypeStruct(inputs.shape, F32)]
            + [jax.ShapeDtypeStruct((2, half, rows, order), F32)] * 2,
            compiler_params=params(),
            cost_estimate=cost(6 * flops, 4 * 2 * (2 * order * order + 3 * count * order)),
            input_output_aliases={} if k == 0 else {1: 0},
        )(ids, before, *args)
        part, last = scatter(odd, even)
        first_parts.append(part)
    second_out = settle(second_parts, input_grad)
    return (input_grad, settle(first_parts, last), second_out)


def solution(mesh):
    placed = (P("tok", "blk"), P("blk", "tok", None), P("blk", "tok", None), P("tok", "blk"))

    return jax.shard_map(
        body,
        mesh=mesh,
        in_specs=placed,
        out_specs=(P("tok", "blk"), P("blk", "tok", None), P("blk", "tok", None)),
        check_vma=False,
    )
```

```python
import functools
import math

import jax
import jax.numpy as jnp
from jax import lax
from jax.experimental import pallas as pl
from jax.experimental.pallas import tpu as pltpu
from jax.sharding import PartitionSpec as P


F32 = jnp.float32
BF16 = jnp.bfloat16
LANES = 128


def split(value):
    high = value.astype(BF16)
    return high, (value - high.astype(F32)).astype(BF16)


def product(left, right, dims):
    def one(a, b):
        return lax.dot_general(a, b, (dims, ((), ())), preferred_element_type=F32)

    return one(left[0], right[1]) + one(left[1], right[0]) + one(left[0], right[0])


PLAIN = ((1,), (0,))
TURNED = ((1,), (1,))


def swap_groups(first, second):
    half = LANES // 2
    low = lax.broadcasted_iota(jnp.int32, first.shape, 1) < half
    return (
        jnp.where(low, first, pltpu.roll(second, half, 1)),
        jnp.where(low, pltpu.roll(first, half, 1), second),
    )


def place_rows(pieces, me, high, low):
    for p, piece in enumerate(pieces):
        rows = piece.shape[0]
        at = pl.ds(pl.multiple_of((me ^ p) * rows, rows), rows)
        h, l = split(piece[...])
        high[at, :] = h
        low[at, :] = l


def place_turned(value, first_shard, me, rows, high, low):
    turned = value.T
    h, l = split(turned)
    for u in range(turned.shape[0] // rows):
        at = pl.ds(pl.multiple_of(((first_shard + u) ^ me) * rows, rows), rows)
        high[at, :] = h[u * rows : (u + 1) * rows]
        low[at, :] = l[u * rows : (u + 1) * rows]


def forward_kernel(T, Z, ids, x_ref, *refs):
    pieces = (refs[:T], refs[T : 2 * T])
    outs = refs[2 * T : 2 * T + Z]
    xh, xl, fh, fl = refs[2 * T + Z :]
    me, z = ids[0], ids[1]
    step = pl.program_id(0)
    blocks, order = fh.shape[0], fh.shape[1]
    each = fh.shape[2] // LANES

    @pl.when(step == 0)
    def _():
        for b in range(blocks):
            at = slice(b * order, (b + 1) * order)
            h, l = split(x_ref[:, at])
            xh[:, at] = h
            xl[:, at] = l

    results = []
    for b in range(blocks):
        place_rows([piece.at[b // 2] for piece in pieces[b % 2]], me, fh.at[b], fl.at[b])
        at = slice(b * order, (b + 1) * order)
        results.append(product((xh[:, at], xl[:, at]), (fh[b], fl[b]), PLAIN))
    for u in range(each):
        distance = lax.rem(step * each + u + Z - z, Z)
        at = slice(u * LANES, (u + 1) * LANES)
        pairs = [
            swap_groups(results[2 * k][:, at], results[2 * k + 1][:, at])
            for k in range(blocks // 2)
        ]
        for c in range(Z):

            @pl.when(distance == c)
            def _():
                for k, pair in enumerate(pairs):
                    for i in range(2):
                        outs[c][i, :, k * LANES : (k + 1) * LANES] = pair[i]


def columns_kernel(chunks, factor_ref, *outs):
    for k in range(chunks):
        for i in range(2):
            for m in range(chunks):
                outs[2 * k + i][m] = factor_ref[2 * m + i, :, k * LANES : (k + 1) * LANES]


def middle_kernel(T, Z, chunks, parts, ids, *refs):
    arrived = refs[:Z]
    refs = refs[Z:]
    pieces = (refs[:T], refs[T : 2 * T])
    cots = refs[2 * T : 2 * T + 2]
    odd, even = refs[2 * T + 2 : 2 * T + 4]
    outs = refs[2 * T + 4 : 2 * T + 4 + Z * parts]
    mh, ml, th, tl, sh, sl, back = refs[2 * T + 4 + Z * parts :]
    me, z = ids[0], ids[1]
    rows = pieces[0][0].shape[0]
    step = pl.program_id(0)

    @pl.when(step == 0)
    def _():
        for c in range(Z):
            source = lax.rem(z + (Z - c), Z)
            for k in range(chunks):
                q = source * chunks + k
                for i in range(2):
                    value = arrived[c][i, :, k * LANES : (k + 1) * LANES]
                    h, l = split(value)
                    at = pl.ds(pl.multiple_of(q * LANES, LANES), LANES)
                    mh[i, :, at] = h
                    ml[i, :, at] = l
                    place_turned(value, q * (LANES // rows), me, rows, th.at[i], tl.at[i])
        back[...] = jnp.zeros_like(back)

    for i in range(2):
        place_rows(pieces[i], me, sh.at[i], sl.at[i])
        factor = (sh[i], sl[i])
        second = product((mh[i], ml[i]), factor, PLAIN)
        cdf = 0.5 * (1.0 + lax.erf(second * (1.0 / math.sqrt(2.0))))
        density = jnp.exp(-0.5 * second * second) * (1.0 / math.sqrt(2.0 * math.pi))
        delta = split(cots[i][...] * (cdf + second * density))
        grad = product((th[i], tl[i]), delta, PLAIN)
        for p in range(T):
            (odd if p % 2 else even)[i, p // 2] = grad[p * rows : (p + 1) * rows]
        back[i] += product(delta, factor, TURNED)

    @pl.when(step == pl.num_programs(0) - 1)
    def _():
        for c in range(Z):
            start = lax.rem(z + c, Z) * chunks
            for h in range(chunks):
                at = pl.ds(pl.multiple_of((start + h) * LANES, LANES), LANES)
                one, two = swap_groups(back[0, :, at], back[1, :, at])
                part, place = divmod(h, chunks // parts)
                outs[c * parts + part][2 * place] = one
                outs[c * parts + part][2 * place + 1] = two


def backward_kernel(T, Z, chunks, tile, ids, _, x_ref, *refs):
    arrived = refs[: Z * chunks]
    refs = refs[Z * chunks :]
    pieces, refs = refs[: 2 * T * chunks], refs[2 * T * chunks :]
    out, odd, even, dh, dl, th, tl, fh, fl = refs
    me, z = ids[0], ids[1]
    rows = pieces[0].shape[1]
    order = x_ref.shape[1] // 2
    step = pl.program_id(0)

    @pl.when(step == 0)
    def _():
        for c in range(Z):
            source = lax.rem(z + (Z - c), Z)
            for k in range(chunks):
                q = source * chunks + k
                at = pl.ds(pl.multiple_of(q * LANES, LANES), LANES)
                for i in range(2):
                    h, l = split(arrived[c * chunks + k][i])
                    dh[i, :, at] = h
                    dl[i, :, at] = l
        for i in range(2):
            for q in range(order // LANES):
                start = i * order + q * LANES
                value = x_ref[:, start : start + LANES]
                place_turned(value, q * (LANES // rows), me, rows, th.at[i], tl.at[i])
        out[...] = jnp.zeros_like(out)

    for i in range(2):
        for h in range(chunks):
            held = pieces[(2 * h + i) * T : (2 * h + i + 1) * T]
            at = slice(h * LANES, (h + 1) * LANES)
            place_rows([p.at[0] for p in held], me, fh.at[i, :, at], fl.at[i, :, at])
        at = pl.ds(pl.multiple_of(step * tile, tile), tile)
        delta = (dh[i, :, at], dl[i, :, at])
        grad = product((th[i], tl[i]), delta, PLAIN)
        for p in range(T):
            (odd if p % 2 else even)[i, p // 2] = grad[p * rows : (p + 1) * rows]
        out[:, i * order : (i + 1) * order] += product(delta, (fh[i], fl[i]), TURNED)


def cost(flops, moved):
    return pl.CostEstimate(flops=flops, bytes_accessed=moved, transcendentals=0)


def params():
    return pltpu.CompilerParams(
        dimension_semantics=("arbitrary",), vmem_limit_bytes=48 * 1024 * 1024
    )


def kernel(*args, **settings):
    return pl.pallas_call(*args, **settings)


def body(inputs, first_factor, second_factor, cotangent):
    T, Z = lax.axis_size("tok"), lax.axis_size("blk")
    LB, rows, order = first_factor.shape
    count = inputs.shape[0]
    group = order // (LB * Z)
    chunks = LB // 2
    width = LB * group
    tile = 256
    steps = order // tile
    half = T // 2
    ids = jnp.stack([lax.axis_index("tok"), lax.axis_index("blk")]).astype(jnp.int32)
    bits = [1 << k for k in range(1, T.bit_length() - 1)]

    def across(value, bit):
        return lax.ppermute(value, "tok", [(d, d ^ bit) for d in range(T)])

    def along(value, c):
        return lax.ppermute(value, "blk", [(d, (d + c) % Z) for d in range(Z)])

    def gather(shards, after=None):
        if after is not None:
            shards, _ = lax.optimization_barrier((shards, after))
        gathered, last = [], []
        for i, shard in enumerate(shards):
            held = {0: shard}
            for bit in bits if i == 0 else bits[::-1]:
                for p, v in list(held.items()):
                    held[p | bit] = across(v, bit)
            last.append(held[T - 2])
            held.update({p | 1: across(v, 1) for p, v in list(held.items())})
            gathered.append([held[p] for p in range(T)])
        return gathered, last

    def scatter(odd, even):
        met = across(odd, 1)
        terms = [
            {p: [(even, (i, p // 2)), (met, (i, p // 2))] for p in range(0, T, 2)}
            for i in range(2)
        ]
        sums = None
        for n in range(len(bits)):
            going, sums = [], []
            for i, bit in enumerate((bits[n], bits[::-1][n])):
                going.append([p for p in terms[i] if p & bit])
                sums.append(jnp.stack([total(terms[i].pop(p)) for p in going[i]]))
            sums = lax.optimization_barrier(sums)
            for i, bit in enumerate((bits[n], bits[::-1][n])):
                sent = across(sums[i], bit)
                for m, p in enumerate(going[i]):
                    terms[i][p ^ bit].append((sent, m))
        return [terms[i][0] for i in range(2)], sums

    def total(found):
        return functools.reduce(jnp.add, [array[at] for array, at in found])

    def settle(parts, after):
        arrays = [[[array for array, _ in found] for found in part] for part in parts]
        arrays, _ = lax.optimization_barrier((arrays, after))
        sums = []
        for part, held in zip(parts, arrays):
            for found, group in zip(part, held):
                sums.append(total([(array, at) for array, (_, at) in zip(group, found)]))
        return jnp.stack(sums)

    def full(shape):
        return pl.BlockSpec(shape, lambda n, ids: (0,) * len(shape))

    halves = kernel(
        functools.partial(columns_kernel, chunks),
        grid=(Z,),
        in_specs=[pl.BlockSpec((LB, rows, width), lambda n: (0, 0, n))],
        out_specs=[pl.BlockSpec((chunks, rows, LANES), lambda n: (0, 0, n))] * LB,
        out_shape=[jax.ShapeDtypeStruct((chunks, rows, Z * LANES), F32)] * LB,
        compiler_params=params(),
    )(first_factor)
    first_pieces, last = [], None
    for k in range(chunks):
        found, ended = gather(halves[2 * k : 2 * k + 2])
        first_pieces.append(found)
        last = ended if last is None else last
    second_pieces = []
    for k in range(chunks):
        shards = [second_factor[2 * k], second_factor[2 * k + 1]]
        second_pieces.append(gather(shards, last)[0])

    flops = 2 * 2 * count * order * order
    column = pl.BlockSpec((rows, tile), lambda n, ids: (0, n))
    each = 2 if Z % 2 == 0 else 1
    mixed = []
    for k in range(chunks):
        sent = kernel(
            functools.partial(forward_kernel, T, Z),
            grid_spec=pltpu.PrefetchScalarGridSpec(
                num_scalar_prefetch=1,
                grid=(Z // each,),
                in_specs=[full((count, LB * order))]
                + [pl.BlockSpec((chunks, rows, each * LANES), lambda n, ids: (0, 0, n))] * (2 * T),
                out_specs=[full((2, count, width))] * Z,
                scratch_shapes=[pltpu.VMEM((count, LB * order), BF16)] * 2
                + [pltpu.VMEM((LB, order, each * LANES), BF16)] * 2,
            ),
            out_shape=[jax.ShapeDtypeStruct((2, count, width), F32)] * Z,
            compiler_params=params(),
            cost_estimate=cost(3 * flops, 4 * 2 * (order * order + 2 * count * order)),
        )(ids, inputs, *first_pieces[k][0], *first_pieces[k][1])
        mixed.append([along(sent[c], c) if c else sent[c] for c in range(Z)])

    returned = []
    second_parts = []
    for k in range(chunks):
        parts = chunks if k == chunks - 1 else 1
        odd, even, *sent = kernel(
            functools.partial(middle_kernel, T, Z, chunks, parts),
            grid_spec=pltpu.PrefetchScalarGridSpec(
                num_scalar_prefetch=1,
                grid=(steps,),
                in_specs=[full((2, count, width))] * Z
                + [column] * (2 * T)
                + [
                    pl.BlockSpec((count, tile), lambda n, ids, b=b: (0, b * steps + n))
                    for b in (2 * k, 2 * k + 1)
                ],
                out_specs=[pl.BlockSpec((2, half, rows, tile), lambda n, ids: (0, 0, 0, n))] * 2
                + [full((LB // parts, count, LANES))] * (Z * parts),
                scratch_shapes=[pltpu.VMEM((2, count, order), BF16)] * 2
                + [pltpu.VMEM((2, order, count), BF16)] * 2
                + [pltpu.VMEM((2, order, tile), BF16)] * 2
                + [pltpu.VMEM((2, count, order), F32)],
            ),
            out_shape=[jax.ShapeDtypeStruct((2, half, rows, order), F32)] * 2
            + [jax.ShapeDtypeStruct((LB // parts, count, LANES), F32)] * (Z * parts),
            compiler_params=params(),
            cost_estimate=cost(9 * flops, 4 * 2 * (2 * order * order + 3 * count * order)),
        )(
            ids,
            *mixed[k],
            *second_pieces[k][0],
            *second_pieces[k][1],
            cotangent,
            cotangent,
        )
        arrived = [[None] * parts for _ in range(Z)]
        for part in range(parts):
            for c in range(Z):
                value = sent[c * parts + part]
                arrived[c][part] = along(value, c) if c else value
        returned.append(arrived)
        second_parts.append(scatter(odd, even)[0])

    def arrivals(pair):
        found = []
        for c in range(Z):
            for arrived in returned:
                parts = arrived[c]
                found.append((parts[pair], 0) if len(parts) > 1 else (parts[0], pair))
        specs = [
            pl.BlockSpec((2, count, LANES), lambda n, ids, at=at: (at, 0, 0)) for _, at in found
        ]
        return [array for array, _ in found], specs

    first_parts = []
    input_grad = None
    for k in range(chunks):
        arrays, specs = arrivals(k)
        pieces = [p for found in first_pieces for held in found for p in held]
        args = (inputs, *arrays, *pieces)
        before = ids if input_grad is None else input_grad
        input_grad, odd, even = kernel(
            functools.partial(backward_kernel, T, Z, chunks, width),
            grid_spec=pltpu.PrefetchScalarGridSpec(
                num_scalar_prefetch=1,
                grid=(Z,),
                in_specs=[pl.BlockSpec(memory_space=pl.ANY)]
                + [pl.BlockSpec((count, 2 * order), lambda n, ids, k=k: (0, k))]
                + specs
                + [pl.BlockSpec((1, rows, LANES), lambda n, ids, k=k: (k, 0, n))] * len(pieces),
                out_specs=[pl.BlockSpec((count, 2 * order), lambda n, ids, k=k: (0, k))]
                + [pl.BlockSpec((2, half, rows, width), lambda n, ids: (0, 0, 0, n))] * 2,
                scratch_shapes=[pltpu.VMEM((2, count, order), BF16)] * 2
                + [pltpu.VMEM((2, order, count), BF16)] * 2
                + [pltpu.VMEM((2, order, width), BF16)] * 2,
            ),
            out_shape=[jax.ShapeDtypeStruct(inputs.shape, F32)]
            + [jax.ShapeDtypeStruct((2, half, rows, order), F32)] * 2,
            compiler_params=params(),
            cost_estimate=cost(6 * flops, 4 * 2 * (2 * order * order + 3 * count * order)),
            input_output_aliases={} if k == 0 else {1: 0},
        )(ids, before, *args)
        part, last = scatter(odd, even)
        first_parts.append(part)
    second_out = settle(second_parts, input_grad)
    return (input_grad, settle(first_parts, last), second_out)


def solution(mesh):
    placed = (P("tok", "blk"), P("blk", "tok", None), P("blk", "tok", None), P("tok", "blk"))

    return jax.shard_map(
        body,
        mesh=mesh,
        in_specs=placed,
        out_specs=(P("tok", "blk"), P("blk", "tok", None), P("blk", "tok", None)),
        check_vma=False,
    )
```
